32 devices in a mesh: row: 4 (over z), col: 8 (over y, x, core).
Axes of the slice: x: 2, y: 2, z: 4, core: 2. Of those that a mesh axis runs over, the one named last changes fastest.
Arguments:
- right_side: float32 [512, 512, 512], P(('row', 'col')), may hold values from -51 to 51
- coupling: float32 [512, 512, 512], P(('row', 'col')), may hold values from 0.01 to 0.3
Outputs:
- solution: float32 [512, 512, 512], P(('row', 'col'))
- residual: float32 [512, 512, 512], P(('row', 'col'))
- residual_norm: float32 [1], replicated
The draws below stay inside these ranges and needn't reach their ends.
All inputs are finite; a program needn't handle non-finite values.
Results may differ from the reference program's by a relative error of at most 0.0003.
Values sent between devices are 32-bit elements; how exact they have to be, the bound alone decides.
A program may use at most 192 MiB of HBM per device.

```python
import math
import jax
import jax.numpy as jnp

NX = 512
NY = 512
NZ = 512


def draw_right_side(key, part):
    base_key = jax.random.fold_in(key, 101)
    first_key, second_key = jax.random.split(base_key)
    plane = jnp.arange(NZ).astype(jnp.float32) / NZ
    zscale = jnp.exp((plane - 0.5) * math.log(10.0))
    xscale = jnp.exp(jax.random.uniform(second_key, (NX,), jnp.float32, -0.5 * math.log(10.0), 0.5 * math.log(10.0)))
    base = jnp.clip(jax.random.normal(first_key, (NZ, NY, NX), jnp.float32), -5.0, 5.0)
    return (base * zscale[:, None, None] * xscale[None, None, :]).astype(jnp.float32)


def levels(rng, extent, shards, low, largest):
    loudness, own = 1.0, jax.random.fold_in(rng, 6)
    for position, blocks in shards:
        steps = jnp.exp(jax.random.uniform(jax.random.fold_in(own, position), (blocks,), jnp.float32, low / len(shards), largest / len(shards)))
        loudness = loudness * jnp.repeat(steps, extent[position] // blocks).reshape([-1 if axis == position else 1 for axis in range(len(extent))])
    return loudness


def setup_inputs(seed: int = 0) -> dict:
    key_of = jax.random.split(jax.random.key(seed), 3)
    return {
        "right_side": draw_right_side(jax.random.fold_in(key_of[2], 71), 0),
        "coupling": jnp.clip(jnp.exp(math.log(0.3) - 3.4011974 * jax.random.uniform(key_of[1], (NZ, NY, NX), jnp.float32) ** levels(key_of[1], (NZ, NY, NX), ((0, 32),), -0.2, 0.2)), 0.01, 0.3),
    }


def hartley(field, axis):
    spectral = jnp.fft.fft(field, axis=axis)
    return jnp.real(spectral) - jnp.imag(spectral)

def wave_square(count):
    index = jnp.arange(count).astype(jnp.int32)
    signed = jnp.where(2 * index < count, index, index - count).astype(jnp.float32)
    return jnp.square(signed * (2.0 * math.pi / count))

def reference(right_side, coupling):
    spectrum = hartley(hartley(hartley(right_side, 2), 1), 0)
    eigen = wave_square(NZ)[:, None, None] + wave_square(NY)[None, :, None] + wave_square(NX)[None, None, :]
    volume = float(NX * NY * NZ)
    positive = eigen > 0
    scaled = jnp.where(positive, spectrum / jnp.where(positive, eigen * volume, 1.0), 0.0)
    solution = hartley(hartley(hartley(scaled, 0), 1), 2)
    lap = 6.0 * solution
    for axis in range(3):
        lap = lap - jnp.roll(solution, 1, axis) - jnp.roll(solution, -1, axis)
    residual = right_side - (coupling * solution + lap)
    residual_norm = jnp.sqrt(jnp.sum(residual * residual)).reshape(1)
    return (solution, residual, residual_norm)
```

```python
import functools
import math

import jax
import jax.numpy as jnp
from jax import lax
from jax.experimental import pallas as pl
from jax.experimental.pallas import tpu as pltpu
from jax.sharding import PartitionSpec as P

HIGH = lax.Precision.HIGH
AXES = ("row", "col")
CHUNKS = 2


def half_tables(count):
    half = count // 2
    index = jnp.arange(half, dtype=jnp.int32)

    def table(frequency):
        product = index[:, None] * frequency[None, :] % count
        angle = product.astype(jnp.float32) * (2.0 * math.pi / count)
        return jnp.cos(angle) + jnp.sin(angle)

    return table(2 * index), table(2 * index + 1)


def wave_square(count):
    half = count // 2
    even = 2 * jnp.arange(half, dtype=jnp.int32)
    index = jnp.concatenate([even, even + 1])
    signed = jnp.where(2 * index < count, index, index - count).astype(jnp.float32)
    return jnp.square(signed * (2.0 * math.pi / count))


LETTERS = ("jbc,jk->kbc", "ajc,jk->akc", "abj,jk->abk")
BACK = ("kbc,jk->jbc", "akc,jk->ajc", "abk,jk->abj")


def halves(field, dim):
    half = field.shape[dim] // 2
    return (
        lax.slice_in_dim(field, 0, half, axis=dim),
        lax.slice_in_dim(field, half, None, axis=dim),
    )


def dot(spec, field, table):
    return jnp.einsum(spec, field, table, precision=HIGH)


def forward(field, tables, dim):
    low, high = halves(field, dim)
    even = dot(LETTERS[dim], low + high, tables[0])
    odd = dot(LETTERS[dim], low - high, tables[1])
    return jnp.concatenate([even, odd], axis=dim)


def inverse(spectrum, tables, dim):
    low, high = halves(spectrum, dim)
    even = dot(BACK[dim], low, tables[0])
    odd = dot(BACK[dim], high, tables[1])
    return jnp.concatenate([even + odd, even - odd], axis=dim)


def split(value):
    high = value.astype(jnp.bfloat16)
    low = (value - high.astype(jnp.float32)).astype(jnp.bfloat16)
    return high, low


def tail_kernel(
    count, per, *refs
):
    slabs, refs = refs[:2 * per], refs[2 * per:]
    below, above, even_ref, odd_ref, right_ref, coupling_ref = refs[:6]
    solution_ref, residual_ref, squares_ref, tables, ring = refs[6:]
    step = pl.program_id(0)

    @pl.when(step == 0)
    def _():
        for which, ref in enumerate((even_ref, odd_ref)):
            high, low = split(ref[...])
            tables[2 * which] = high
            tables[2 * which + 1] = low
        squares_ref[...] = jnp.zeros_like(squares_ref)

    def transform(value, which):
        high, low = split(value)
        total = jnp.dot(low, tables[2 * which], preferred_element_type=jnp.float32)
        total += jnp.dot(high, tables[2 * which + 1], preferred_element_type=jnp.float32)
        return total + jnp.dot(high, tables[2 * which], preferred_element_type=jnp.float32)

    def plane(even, odd):
        first = transform(even, 0)
        second = transform(odd, 1)
        half = first.shape[1]
        slot = ring.at[lax.rem(step, 3)]
        slot[:, :half] = first + second
        slot[:, half:] = first - second

    @pl.when(step == 0)
    def _():
        plane(below[0], below[1])

    @pl.when(step == count + 1)
    def _():
        plane(above[0], above[1])

    @pl.when((step > 0) & (step <= count))
    def _():
        parts = [ref[0] for ref in slabs]
        if per == 1:
            plane(parts[0], parts[1])
        else:
            plane(jnp.concatenate(parts[:per], axis=1), jnp.concatenate(parts[per:], axis=1))
        solution_ref[0] = ring[lax.rem(step, 3)]

    @pl.when(step > 1)
    def _():
        here = ring[lax.rem(step - 1, 3)]
        rows, cols = here.shape
        lap = 6.0 * here - ring[lax.rem(step, 3)] - ring[lax.rem(step - 2, 3)]
        lap = lap - pltpu.roll(here, 1, 0) - pltpu.roll(here, rows - 1, 0)
        lap = lap - pltpu.roll(here, 1, 1) - pltpu.roll(here, cols - 1, 1)
        residual = right_ref[0] - (coupling_ref[0] * here + lap)
        residual_ref[0] = residual
        squares_ref[...] += jnp.sum(residual * residual, axis=0, keepdims=True)


def tail(slabs, below, above, tables, right_side, coupling):
    planes, rows, cols = right_side.shape
    per = len(slabs) // 2

    def clip(shift):
        return lambda t: (jnp.clip(t - shift, 0, planes - 1), 0, 0)

    def whole(shape):
        return pl.BlockSpec(shape, lambda t: (0,) * len(shape))

    block = (1, rows, cols)
    return pl.pallas_call(
        functools.partial(tail_kernel, planes, per),
        grid=(planes + 2,),
        in_specs=[pl.BlockSpec((1, rows, part.shape[2]), clip(1)) for part in slabs]
        + [whole(below.shape), whole(above.shape), whole(tables[0].shape), whole(tables[1].shape)]
        + [pl.BlockSpec(block, clip(2)), pl.BlockSpec(block, clip(2))],
        out_specs=[pl.BlockSpec(block, clip(1)), pl.BlockSpec(block, clip(2)), whole((1, cols))],
        out_shape=[
            jax.ShapeDtypeStruct(right_side.shape, jnp.float32),
            jax.ShapeDtypeStruct(right_side.shape, jnp.float32),
            jax.ShapeDtypeStruct((1, cols), jnp.float32),
        ],
        scratch_shapes=[
            pltpu.VMEM((4,) + tables[0].shape, jnp.bfloat16),
            pltpu.VMEM((3, rows, cols), jnp.float32),
        ],
        compiler_params=pltpu.CompilerParams(vmem_limit_bytes=48 * 1024 * 1024),
        name="tail",
    )(*slabs, below, above, tables[0], tables[1], right_side, coupling)


def twice(left, right):
    total = jnp.dot(left[1], right[0], preferred_element_type=jnp.float32)
    total += jnp.dot(left[0], right[1], preferred_element_type=jnp.float32)
    return total + jnp.dot(left[0], right[0], preferred_element_type=jnp.float32)


def keep(tables, refs):
    for position, ref in enumerate(refs):
        high, low = split(ref[...])
        tables[2 * position] = high
        tables[2 * position + 1] = low


def pair(tables, position):
    return tables[2 * position], tables[2 * position + 1]


def plane_kernel(sign, right_ref, x_ref, even_ref, odd_ref, out_ref, x_table, y_tables):
    @pl.when(pl.program_id(0) == 0)
    def _():
        keep(x_table, (x_ref,))
        keep(y_tables, (even_ref, odd_ref))

    field = right_ref[0]
    rows, cols = field.shape
    lines = twice(split(field[:, :cols // 2] + sign * field[:, cols // 2:]), pair(x_table, 0))
    low, high = lines[:rows // 2], lines[rows // 2:]
    ranks, _, width, half = out_ref.shape
    shape = (ranks // 2, width, half)
    out_ref[:ranks // 2, 0] = twice(pair(y_tables, 0), split(low + high)).reshape(shape)
    out_ref[ranks // 2:, 0] = twice(pair(y_tables, 1), split(low - high)).reshape(shape)


def whole(shape):
    return pl.BlockSpec(shape, lambda *_: (0,) * len(shape))


LIMIT = pltpu.CompilerParams(vmem_limit_bytes=56 * 1024 * 1024)


def planes_forward(right_side, sign, table_x, tables_y, ranks):
    planes, rows, cols = right_side.shape
    width, half = rows // ranks, cols // 2
    return pl.pallas_call(
        functools.partial(plane_kernel, sign),
        grid=(planes,),
        in_specs=[pl.BlockSpec((1, rows, cols), lambda t: (t, 0, 0)), whole(table_x.shape)]
        + [whole(table.shape) for table in tables_y],
        out_specs=pl.BlockSpec((ranks, 1, width, half), lambda t: (0, t, 0, 0)),
        out_shape=jax.ShapeDtypeStruct((ranks, planes, width, half), jnp.float32),
        scratch_shapes=[
            pltpu.VMEM((2,) + table_x.shape, jnp.bfloat16),
            pltpu.VMEM((4,) + tables_y[0].shape, jnp.bfloat16),
        ],
        compiler_params=LIMIT,
        cost_estimate=pl.CostEstimate(
            flops=12 * planes * rows * half * half,
            bytes_accessed=6 * planes * rows * cols, transcendentals=0,
        ),
        name="planes_forward",
    )(right_side, table_x, *tables_y)


def line_kernel(volume, pencil_ref, rows_ref, z_ref, x_ref, *refs):
    *table_refs, out_ref, tables = refs
    lane = pl.program_id(1)

    @pl.when((lane == 0) & (pl.program_id(0) == 0))
    def _():
        keep(tables, table_refs)

    depth, group, span = pencil_ref.shape
    half = depth // 2
    source = pencil_ref.reshape(depth * group, span)
    target = out_ref.reshape(depth * group, span)

    def scale(spectrum, wave_z, row):
        eigen = wave_z + row + x_ref[...]
        positive = eigen > 0
        return jnp.where(positive, spectrum / jnp.where(positive, eigen * volume, 1.0), 0.0)

    def body(index, carry):
        low = source[pl.ds(index, half, stride=group), :]
        high = source[pl.ds(index + half * group, half, stride=group), :]
        row = rows_ref[pl.program_id(0) * group + index]
        even = scale(twice(pair(tables, 0), split(low + high)), z_ref[:half], row)
        odd = scale(twice(pair(tables, 1), split(low - high)), z_ref[half:], row)
        first = twice(pair(tables, 2), split(even))
        second = twice(pair(tables, 3), split(odd))
        target[pl.ds(index, half, stride=group), :] = first + second
        target[pl.ds(index + half * group, half, stride=group), :] = first - second
        return carry

    lax.fori_loop(0, group, body, 0)


def lines_solved(pencil, wave_rows, wave_z, wave_x, tables, volume):
    depth, width, span = pencil.shape
    group, lanes = 8, 128
    transposed = (tables[0].T, tables[1].T) + tuple(tables)
    block = pl.BlockSpec((depth, group, lanes), lambda y, x: (0, y, x))
    return pl.pallas_call(
        functools.partial(line_kernel, volume),
        grid=(width // group, span // lanes),
        in_specs=[
            block,
            pl.BlockSpec(memory_space=pltpu.SMEM),
            whole((depth, 1)),
            pl.BlockSpec((1, lanes), lambda y, x: (0, x)),
        ]
        + [whole(table.shape) for table in transposed],
        out_specs=block,
        out_shape=jax.ShapeDtypeStruct(pencil.shape, jnp.float32),
        scratch_shapes=[pltpu.VMEM((8,) + tables[0].shape, jnp.bfloat16)],
        compiler_params=LIMIT,
        cost_estimate=pl.CostEstimate(
            flops=12 * depth * width * span * depth,
            bytes_accessed=8 * depth * width * span, transcendentals=0,
        ),
        name="lines_solved",
    )(pencil, wave_rows, wave_z[:, None], wave_x[None], *transposed)


def shards(right_side, coupling):
    planes, rows, cols = right_side.shape
    ranks = lax.axis_size("row") * lax.axis_size("col")
    depth = planes * ranks
    tables_x = half_tables(cols)
    tables_y = half_tables(rows)
    tables_z = half_tables(depth)
    block = lax.axis_index(AXES)
    width = rows // ranks
    wave_rows = lax.dynamic_slice_in_dim(wave_square(rows), block * width, width, 0)
    wave_z = wave_square(depth)
    wave_x = wave_square(cols)
    volume = float(depth * rows * cols)

    low, high = halves(right_side, 2)
    parts = (low + high, low - high)
    span = cols // CHUNKS
    per = CHUNKS // 2
    slabs = []
    for chunk in range(CHUNKS):
        which, piece = divmod(chunk, per)
        columns = tables_x[which][:, piece * span:(piece + 1) * span]
        waves = wave_x[chunk * span:(chunk + 1) * span]
        if width % 8 == 0:
            sides = (tables_y[0].T, tables_y[1].T)
            spectra = planes_forward(right_side, 1.0 - 2.0 * which, columns, sides, ranks)
            pencil = lax.all_to_all(spectra, AXES, split_axis=0, concat_axis=0, tiled=True)
            pencil = pencil.reshape(depth, width, span)
            lines = lines_solved(pencil, wave_rows, wave_z, waves, tables_z, volume)
            lines = lines.reshape(ranks, planes, width, span)
            slab = lax.all_to_all(lines, AXES, split_axis=0, concat_axis=0, tiled=True)
            slab = slab.transpose(1, 0, 2, 3).reshape(planes, rows, span)
        else:
            spectra = forward(dot(LETTERS[2], parts[which], columns), tables_y, 1)
            pencil = lax.all_to_all(spectra, AXES, split_axis=1, concat_axis=0, tiled=True)
            spectrum = forward(pencil, tables_z, 0)
            eigen = wave_z[:, None, None] + wave_rows[None, :, None] + waves[None, None, :]
            positive = eigen > 0
            scaled = jnp.where(positive, spectrum / jnp.where(positive, eigen * volume, 1.0), 0.0)
            lines = inverse(scaled, tables_z, 0)
            slab = lax.all_to_all(lines, AXES, split_axis=0, concat_axis=1, tiled=True)
        slabs.append(inverse(slab, tables_y, 1))
    count = ranks
    ahead = [(i, (i + 1) % count) for i in range(count)]
    behind = [(target, source) for source, target in ahead]

    def edge(index, ring):
        parts = [lax.slice_in_dim(part, index, index + 1, axis=0) for part in slabs]
        even = jnp.concatenate(parts[:per], axis=2)
        odd = jnp.concatenate(parts[per:], axis=2)
        return lax.ppermute(jnp.concatenate([even, odd], axis=0), AXES, ring)

    below = edge(planes - 1, ahead)
    above = edge(0, behind)
    back = (tables_x[0].T, tables_x[1].T)
    answer, residual, partial = tail(slabs, below, above, back, right_side, coupling)
    squares = lax.psum(jnp.sum(partial), AXES)
    return (answer, residual, jnp.sqrt(squares).reshape(1))


def solution(mesh):
    spec = P(AXES, None, None)
    return jax.shard_map(
        shards, mesh=mesh, in_specs=(spec, spec), out_specs=(spec, spec, P()), check_vma=False
    )
```
